32 devices in a mesh: dp: 1 (over z), fsdp: 32 (over y, x, core).
Axes of the slice: x: 4, y: 4, z: 1, core: 2. Of those that a mesh axis runs over, the one named last changes fastest.
The devices are a block of a 4x4x8 slice.
Arguments:
- tokens: bfloat16 [256, 128, 7168], P(('dp', 'fsdp'))
- gain_in: bfloat16 [7168], P('fsdp')
- w_dq: bfloat16 [7168, 1536], P('fsdp')
- gain_q: bfloat16 [1536], P('fsdp')
- w_uq: bfloat16 [1536, 12288], P('fsdp')
- w_dkv: bfloat16 [7168, 576], P('fsdp')
- gain_kv: bfloat16 [512], P('fsdp')
- w_ukv: bfloat16 [512, 16384], P('fsdp')
- w_out: bfloat16 [8192, 7168], P('fsdp')
Outputs:
- output 1: bfloat16 [256, 128, 7168], P(('dp', 'fsdp'))
- output 2: bfloat16 [256, 128, 512], P(('dp', 'fsdp'))
- output 3: bfloat16 [256, 128, 64], P(('dp', 'fsdp'))
All inputs are finite; a program needn't handle non-finite values.
Results may differ from the reference program's by a relative error of at most 0.00639726.
Values are sent between devices in bfloat16 or wider.
A program may use at most 768 MiB of HBM per device.

```python
import jax
import jax.numpy as jnp
from jax import lax

PROMPTS = 256
SEQ_LEN = 128
D_MODEL = 7168
N_HEADS = 64
Q_RANK = 1536
KV_RANK = 512
NOPE_DIM = 128
ROPE_DIM = 64
V_DIM = 128
EPSILON = 1e-6
ROPE_THETA = 10000.0


def setup_inputs(seed: int = 0, part: int = 0) -> dict:
    key_list = jax.random.split(jax.random.key(seed), 9)

    def draw_weight(sub_key, n_rows, n_cols):
        drawn = jax.random.normal(sub_key, (n_rows, n_cols), jnp.float32) * (n_rows ** -0.5)
        return drawn.astype(jnp.bfloat16)

    def draw_gain(sub_key, n_items, centre):
        drawn = centre * (1.0 + 0.3 * jax.random.normal(sub_key, (n_items,), jnp.float32))
        return drawn.astype(jnp.bfloat16)

    tok_key = jax.random.fold_in(key_list[0], part)
    tokens = jax.random.normal(tok_key, (PROMPTS, SEQ_LEN, D_MODEL), jnp.float32).astype(jnp.bfloat16)
    return {
        'tokens': tokens,
        'gain_in': draw_gain(key_list[1], D_MODEL, 1.0),
        'w_dq': draw_weight(key_list[2], D_MODEL, Q_RANK),
        'gain_q': draw_gain(key_list[3], Q_RANK, 2.0),
        'w_uq': draw_weight(key_list[4], Q_RANK, N_HEADS * (NOPE_DIM + ROPE_DIM)),
        'w_dkv': draw_weight(key_list[5], D_MODEL, KV_RANK + ROPE_DIM),
        'gain_kv': draw_gain(key_list[6], KV_RANK, 1.0),
        'w_ukv': draw_weight(key_list[7], KV_RANK, N_HEADS * (NOPE_DIM + V_DIM)),
        'w_out': draw_weight(key_list[8], N_HEADS * V_DIM, D_MODEL),
    }


def rms_scale(values_in, gain_vec):
    values_f32 = values_in.astype(jnp.float32)
    inv_rms = lax.rsqrt(jnp.mean(values_f32 * values_f32, axis=-1, keepdims=True) + EPSILON)
    return values_f32 * inv_rms * gain_vec.astype(jnp.float32)


def rope_tables():
    half_dim = ROPE_DIM // 2
    inv_freq = ROPE_THETA ** (-2.0 * jnp.arange(half_dim, dtype=jnp.float32) / ROPE_DIM)
    angles = jnp.arange(SEQ_LEN, dtype=jnp.float32)[:, None] * inv_freq[None, :]
    return jnp.cos(angles), jnp.sin(angles)


def apply_rope(values_in, cos_t, sin_t):
    half_dim = values_in.shape[-1] // 2
    lo_half = values_in[..., :half_dim]
    hi_half = values_in[..., half_dim:]
    return jnp.concatenate([lo_half * cos_t - hi_half * sin_t, hi_half * cos_t + lo_half * sin_t], axis=-1)


def one_prompt(tok_rows, gain_in, w_dq, gain_q, w_uq, w_dkv, gain_kv, w_ukv, w_out):
    cos_t, sin_t = rope_tables()
    normed = rms_scale(tok_rows, gain_in).astype(jnp.bfloat16)
    q_down = jnp.dot(normed, w_dq, preferred_element_type=jnp.float32)
    q_lat = rms_scale(q_down, gain_q).astype(jnp.bfloat16)
    q_full = jnp.dot(q_lat, w_uq, preferred_element_type=jnp.float32).reshape(SEQ_LEN, N_HEADS, NOPE_DIM + ROPE_DIM)
    q_nope = q_full[:, :, :NOPE_DIM].astype(jnp.bfloat16)
    q_pe = apply_rope(q_full[:, :, NOPE_DIM:], cos_t[:, None, :], sin_t[:, None, :]).astype(jnp.bfloat16)
    kv_down = jnp.dot(normed, w_dkv, preferred_element_type=jnp.float32)
    latent = rms_scale(kv_down[:, :KV_RANK], gain_kv).astype(jnp.bfloat16)
    k_pe = apply_rope(kv_down[:, KV_RANK:], cos_t, sin_t).astype(jnp.bfloat16)
    kv_up = jnp.dot(latent, w_ukv, preferred_element_type=jnp.float32).astype(jnp.bfloat16)
    kv_up = kv_up.reshape(SEQ_LEN, N_HEADS, NOPE_DIM + V_DIM)
    k_nope = kv_up[:, :, :NOPE_DIM].astype(jnp.float32)
    values = kv_up[:, :, NOPE_DIM:].astype(jnp.float32)
    score_scale = (NOPE_DIM + ROPE_DIM) ** -0.5
    scores = jnp.einsum('qhd,khd->hqk', q_nope.astype(jnp.float32), k_nope)
    scores = scores + jnp.einsum('qhd,kd->hqk', q_pe.astype(jnp.float32), k_pe.astype(jnp.float32))
    causal = jnp.arange(SEQ_LEN)[:, None] >= jnp.arange(SEQ_LEN)[None, :]
    scores = jnp.where(causal[None, :, :], scores * score_scale, -1e30)
    attn_probs = jax.nn.softmax(scores, axis=-1).astype(jnp.bfloat16)
    attn_out = jnp.einsum('hqk,khd->qhd', attn_probs.astype(jnp.float32), values).astype(jnp.bfloat16)
    attn_out = attn_out.reshape(SEQ_LEN, N_HEADS * V_DIM)
    proj_out = jnp.dot(attn_out, w_out, preferred_element_type=jnp.float32)
    y_rows = (tok_rows.astype(jnp.float32) + proj_out).astype(jnp.bfloat16)
    return y_rows, latent, k_pe


def reference(tokens, gain_in, w_dq, gain_q, w_uq, w_dkv, gain_kv, w_ukv, w_out):
    def per_prompt(tok_rows):
        return one_prompt(tok_rows, gain_in, w_dq, gain_q, w_uq, w_dkv, gain_kv, w_ukv, w_out)

    y_out, kv_cache, pe_cache = lax.map(per_prompt, tokens)
    return (y_out, kv_cache, pe_cache)
```

```python
import math

import jax
import jax.numpy as jnp
import numpy as np
from jax import lax
from jax.experimental import pallas as pl
from jax.experimental.pallas import tpu as pltpu
from jax.sharding import PartitionSpec as P

EPSILON = 1e-6
ROPE_THETA = 10000.0
NEG = -1e30
MESH = pl.DeviceIdType.MESH
F32 = jnp.float32
BF16 = jnp.bfloat16
LANES = 128
CORES = 2
GROUP_HEADS = 8
HALF = 4
WIDE = 512
NARROW = 256
ROWS = 256
HROWS = 512


def rope_tables(seq_len, rope_dim):
    half = rope_dim // 2
    inv_freq = ROPE_THETA ** (-2.0 * np.arange(half) / rope_dim)
    angles = np.arange(seq_len)[:, None] * inv_freq[None, :]
    cos, sin, zero = np.cos(angles), np.sin(angles), np.zeros_like(angles)
    reps = LANES // rope_dim
    c = np.tile(np.concatenate([cos, cos], 1), (1, reps))
    lo = np.tile(np.concatenate([-sin, zero], 1), (1, reps))
    hi = np.tile(np.concatenate([zero, sin], 1), (1, reps))
    return [t.astype(np.float32) for t in (c, lo, hi)]


def inv_rms(v, n):
    return lax.rsqrt(jnp.sum(v * v, axis=-1, keepdims=True) * (1.0 / n) + EPSILON)


class Chunk:
    def __init__(self, cid, kind, own, full, rows, col, width):
        self.cid, self.kind, self.own, self.full = cid, kind, own, full
        self.rows, self.cols = rows, pl.ds(col, width)


def make_kernel(n_dev, dims):
    side = math.isqrt(n_dev // CORES)
    (T, D, QR, KVR, H, NOPE, RD, VD, SEQ) = dims
    GW = GROUP_HEADS * (NOPE + RD)
    KVW = GROUP_HEADS * (NOPE + VD)
    n_groups = H // GROUP_HEADS
    r_d, r_q, r_kv, r_o = D // n_dev, QR // n_dev, KVR // n_dev, H * VD // n_dev
    scale = (NOPE + RD) ** -0.5
    half = RD // 2
    n_wide = D // (2 * WIDE) - 1

    def kernel(x, gp, wdkv, wdq, wuq, wukv, wo, tc, tlo, thi, cmask, lmask,
               y, lat, kpe, g_gp, g_dkv, g_dq, g_uq, g_ukv, g_o,
               act, cq, cl, rr, qdown, wbuf, xst, wq, wkv, qn, qp, kv, ys, gv,
               st_gp, st_dkv, st_dq, st_uq, st_ukv,
               send, recv, loc, stg, wsem, psem, xsem, ysem):
        me = lax.axis_index("fsdp")
        core = lax.rem(me, CORES)
        px = lax.rem(me // CORES, side)
        py = me // (CORES * side)
        up = lambda v, d: lax.rem(v + d, side)
        dev = lambda yy, xx, kk: {"fsdp": (yy * side + xx) * CORES + kk}
        partner = dev(py, px, 1 - core)

        barrier = pltpu.get_barrier_semaphore()
        near = [dev(py, up(px, 1), core), dev(py, up(px, side - 1), core),
                dev(up(py, 1), px, core), dev(up(py, side - 1), px, core), partner]
        for d in near:
            pl.semaphore_signal(barrier, inc=1, device_id=d, device_id_type=MESH)

        n_o = wo.shape[1] // WIDE
        stage_in, stage_out = [], []
        moves = [(gp, st_gp, g_gp), (wdkv, st_dkv, g_dkv), (wdq, st_dq, g_dq),
                 (wuq, st_uq, g_uq), (wukv, st_ukv, g_ukv)]
        for i, (own, st, full) in enumerate(moves):
            stage_in.append(pltpu.make_async_copy(own, st, stg.at[0, i]))
            stage_out.append(pltpu.make_async_copy(st, full.at[py, px, core], stg.at[1, i]))
        for j in range(n_o):
            c = pl.ds(j * WIDE, WIDE)
            stage_in.append(pltpu.make_async_copy(wo.at[:, c], wbuf.at[0, j], stg.at[0, len(moves) + j]))
            stage_out.append(pltpu.make_async_copy(wbuf.at[0, j], g_o.at[py, px, core, :, c], stg.at[1, len(moves) + j]))
        for c in stage_in:
            c.start()
        pl.semaphore_wait(barrier, len(near))

        rounds = [[("A", gp, g_gp, 16, 0, gp.shape[1]), ("A", wdkv, g_dkv, r_d, 0, wdkv.shape[1]),
                   ("B", wdq, g_dq, r_d, 0, WIDE)],
                  [("A", wdq, g_dq, r_d, WIDE, WIDE), ("B", wdq, g_dq, r_d, 2 * WIDE, WIDE)]]
        for g in range(0, n_groups, 2):
            rounds.append([("A", wuq, g_uq, r_q, g * GW, GW), ("A", wukv, g_ukv, r_kv, g * KVW, KVW),
                           ("B", wuq, g_uq, r_q, (g + 1) * GW, GW), ("B", wukv, g_ukv, r_kv, (g + 1) * KVW, KVW)])
        first_o = len(rounds)
        cid, fixed = 0, []
        for r in rounds:
            fixed.append([Chunk(cid + i, *c) for i, c in enumerate(r)])
            cid += len(r)
        last_wide = first_o + n_wide
        n_rounds = last_wide + 2

        def span_o(t, i, wide):
            if wide:
                return pl.multiple_of(((t - first_o) * 2 + i) * WIDE, WIDE), WIDE
            return pl.multiple_of(n_wide * 2 * WIDE + ((t - last_wide) * 2 + i) * NARROW, NARROW), NARROW

        def chunks(t, wide):
            if isinstance(t, int) and t < first_o:
                return fixed[t]
            return [Chunk(cid + (t - first_o) * 2 + i, k, wo, g_o, r_o, *span_o(t, i, wide)) for i, k in enumerate("AB")]

        def in_round(t, fn):
            if isinstance(t, int):
                if 0 <= t < n_rounds:
                    fn(t < last_wide)
            else:
                pl.when(t < last_wide)(lambda: fn(True))

                @pl.when(t >= last_wide)
                def _():
                    pl.when(t < n_rounds)(lambda: fn(False))

        every = slice(None)

        def copy_of(c, j):
            f, s = (px, py) if c.kind == "A" else (py, px)
            h = c.rows // 2
            top, bot = pl.ds(0, h), pl.ds(h, h)

            def block(b, a, rows=every):
                yy, xx = (b, a) if c.kind == "A" else (a, b)
                return c.full.at[yy, xx, core, rows, c.cols]

            def near_by(b, a):
                yy, xx = (b, a) if c.kind == "A" else (a, b)
                return dev(yy, xx, core)

            back = side - 1
            src = None
            if j == 0:
                src, dst, to = c.own.at[:, c.cols], block(s, f), near_by(s, up(f, 1))
            elif j == 1:
                src, dst, to = c.own.at[:, c.cols], block(s, f), near_by(s, up(f, back))
            elif j == 2:
                dst, to = block(s, up(f, back), top), near_by(s, up(f, 1))
            elif j == 3:
                dst, to = block(s, up(f, 1), bot), near_by(s, up(f, back))
            elif j == 4:
                dst, to = block(s, every), near_by(up(s, 1), f)
            elif j == 5:
                dst, to = block(s, every), near_by(up(s, back), f)
            elif j == 6:
                dst, to = block(up(s, back), every, top), near_by(up(s, 1), f)
            elif j == 7:
                dst, to = block(up(s, 1), every, bot), near_by(up(s, back), f)
            else:
                dst, to = block(up(s, (0, back, 1, 2)[j - 8]), every), partner
            return pltpu.make_async_remote_copy(src_ref=dst if src is None else src, dst_ref=dst,
                                                send_sem=send.at[c.cid, j], recv_sem=recv.at[c.cid, j],
                                                device_id=to, device_id_type=MESH)

        def steps(c, names):
            for n in names:
                if n < 0:
                    copy_of(c, ~n).wait_recv()
                else:
                    copy_of(c, n).start()

        S1, S2, S3 = (0, 1), (~0, 2, ~1, 3), (~2, ~3, 4, 5, 8)
        S4, S5, S6 = (~4, 6, 9, ~5, 7, 10), (~6, ~7, 11), (~8, ~9, ~10, ~11)

        def comm(t, names):
            def run(wide):
                for c in chunks(t, wide):
                    steps(c, names)
            in_round(t, run)

        def rows_of(m, n):
            return pl.ds(pl.multiple_of(m * n, n), n)

        def rope(v):
            return v * tc[...] + pltpu.roll(v, LANES - half, 1) * tlo[...] + pltpu.roll(v, half, 1) * thi[...]

        def gain_rows(row, count):
            part = count // n_dev
            width = math.lcm(part, LANES)
            period = width // part
            out = []
            for g in range(n_dev // period):
                tot = None
                for j in range(period):
                    i = g * period + j
                    v = gv[i // (side * CORES), (i // CORES) % side, i % CORES, :, :width].astype(F32)
                    tot = v if tot is None else tot + v
                out.append(tot[row:row + 1, :])
            return out, width

        def norm_tokens():
            cp = pltpu.make_async_copy(g_gp, gv, loc.at[0])
            cp.start()
            xrows = xst.shape[1]
            n = T // xrows
            load = lambda i, slot: pltpu.make_async_copy(x.at[rows_of(i, xrows), :], xst.at[slot], xsem.at[slot])
            load(0, 0).start()
            cp.wait()
            gains, width = gain_rows(0, D)

            @pl.loop(0, n, step=2)
            def _(i0):
                for slot in range(2):
                    i = i0 + slot
                    if slot == 0:
                        load(i + 1, 1).start()
                    else:
                        @pl.when(i + 1 < n)
                        def _():
                            load(i + 1, 0).start()
                    load(i, slot).wait()
                    ss = jnp.zeros((xrows, 1), F32)
                    for g in range(len(gains)):
                        v = xst[slot, :, g * width:(g + 1) * width].astype(F32)
                        ss = ss + jnp.sum(v * v, axis=-1, keepdims=True)
                    inv = lax.rsqrt(ss * (1.0 / D) + EPSILON)
                    for g in range(len(gains)):
                        v = xst[slot, :, g * width:(g + 1) * width].astype(F32)
                        act[rows_of(i, xrows), g * width:(g + 1) * width] = (v * inv * gains[g]).astype(BF16)

        def fetch_d(full, rows, col, width, slot):
            cps = []
            for yy in range(side):
                for xx in range(side):
                    i = (yy * side + xx) * CORES
                    cps.append(pltpu.make_async_copy(full.at[yy, xx, :, :, pl.ds(col, width)],
                                                     wbuf.at[slot, pl.ds(i, CORES), pl.ds(0, rows), pl.ds(0, width)],
                                                     wsem.at[slot, yy * side + xx]))
            return cps

        def start(cps):
            for c in cps:
                c.start()

        def wait(cps):
            for c in cps:
                c.wait()

        def kv_down():
            cps = fetch_d(g_dkv, r_d, 0, KVR, 0) + fetch_d(g_dkv, r_d, KVR, LANES, 1)
            start(cps)
            wait(cps)
            gains, width = gain_rows(2, KVR)
            gain = jnp.concatenate(gains, axis=1)

            @pl.loop(0, T // ROWS)
            def _(m):
                r = rows_of(m, ROWS)
                u = jnp.dot(act[r, :D], wbuf[0, :, :r_d, :].reshape(D, WIDE), preferred_element_type=F32)
                cl[r, :] = (u * inv_rms(u, KVR) * gain).astype(BF16)
                v = jnp.dot(act[r, :D], wbuf[1, :, :r_d, :LANES].reshape(D, LANES), preferred_element_type=F32)
                for b in range(ROWS // SEQ):
                    rr[pl.ds(pl.multiple_of(m * ROWS + b * SEQ, SEQ), SEQ), :] = rope(v[b * SEQ:(b + 1) * SEQ]).astype(BF16)
            pltpu.make_async_copy(cl, lat, loc.at[1]).start()
            pltpu.make_async_copy(rr, kpe, loc.at[2]).start()

        def q_down(j):
            slot = j % 2
            wait(fetch_d(g_dq, r_d, j * WIDE, WIDE, slot))

            @pl.loop(0, T // ROWS)
            def _(m):
                r = rows_of(m, ROWS)
                qdown[r, j * WIDE:(j + 1) * WIDE] = jnp.dot(act[r, :D], wbuf[slot, :, :r_d, :].reshape(D, WIDE),
                                                           preferred_element_type=F32)
            if j == QR // WIDE - 1:
                gains, width = gain_rows(1, QR)

                @pl.loop(0, T // LANES)
                def _(m):
                    r = rows_of(m, LANES)
                    inv = inv_rms(qdown[r, :], QR)
                    for g in range(len(gains)):
                        c = slice(g * width, (g + 1) * width)
                        cq[r, c] = (qdown[r, c] * inv * gains[g]).astype(BF16)

        def fetch_u(i):
            slot = lax.rem(i, 2)
            wa, wb = HALF * (NOPE + RD), HALF * (NOPE + VD)
            ca, cb = pl.ds(pl.multiple_of(i * wa, wa), wa), pl.ds(pl.multiple_of(i * wb, wb), wb)
            return [pltpu.make_async_copy(g_uq.at[:, :, :, :, ca], wq.at[slot], psem.at[0, slot]),
                    pltpu.make_async_copy(g_ukv.at[:, :, :, :, cb], wkv.at[slot], psem.at[1, slot])]

        def heads(i, more):
            slot = lax.rem(i, 2)

            @pl.when(more)
            def _():
                start(fetch_u(i + 1))
            wait(fetch_u(i))
            lo = lmask[0].astype(F32) > 0.5
            pw = 2 * (NOPE + RD)

            @pl.loop(0, T // HROWS)
            def _(m):
                c = cq[rows_of(m, HROWS), :]
                for p in range(HALF // 2):
                    v = jnp.dot(c, wq[slot, :, :, :, :, p * pw:(p + 1) * pw].reshape(QR, pw), preferred_element_type=F32)
                    v0, v1, v2 = (v[:, k * LANES:(k + 1) * LANES] for k in range(3))
                    qn[:, (2 * p) * NOPE:(2 * p + 1) * NOPE] = v0.astype(BF16)
                    qn[:, (2 * p + 1) * NOPE:(2 * p + 2) * NOPE] = pltpu.roll(jnp.where(lo, v2, v1), RD, 1).astype(BF16)
                    pe = jnp.where(lo, v1, v2)
                    for b in range(HROWS // SEQ):
                        rb = slice(b * SEQ, (b + 1) * SEQ)
                        qp[rb, p * LANES:(p + 1) * LANES] = rope(pe[rb]).astype(BF16)
                kv[...] = jnp.dot(cl[rows_of(m, HROWS), :], wkv[slot].reshape(KVR, HALF * (NOPE + VD)),
                                  preferred_element_type=F32).astype(BF16)
                units = [(b, h) for b in range(HROWS // SEQ) for h in range(HALF)]
                visible = cmask[...] > 0.5
                prompt = lambda b: pl.ds(pl.multiple_of(m * HROWS + b * SEQ, SEQ), SEQ)

                def score(b, h):
                    rb = slice(b * SEQ, (b + 1) * SEQ)
                    k0 = h * (NOPE + VD)
                    q_cat = jnp.concatenate([qn[rb, h * NOPE:(h + 1) * NOPE],
                                             qp[rb, (h // 2) * LANES:(h // 2 + 1) * LANES]], axis=1)
                    k_cat = jnp.concatenate([kv[rb, k0:k0 + NOPE], rr[prompt(b), :] * lmask[h % 2]], axis=1)
                    return lax.dot_general(q_cat, k_cat, (((1,), (1,)), ((), ())), preferred_element_type=F32)

                ss = [jnp.where(visible, score(b, h) * scale, NEG) for b, h in units]
                es = [jnp.exp(v - jnp.max(v, axis=-1, keepdims=True)) for v in ss]
                ps = [(e * (1.0 / jnp.sum(e, axis=-1, keepdims=True))).astype(BF16) for e in es]
                for pr, (b, h) in zip(ps, units):
                    v0 = h * (NOPE + VD) + NOPE
                    o = jnp.dot(pr, kv[b * SEQ:(b + 1) * SEQ, v0:v0 + VD], preferred_element_type=F32)
                    act[prompt(b), pl.ds(pl.multiple_of((i * HALF + h) * VD, VD), VD)] = o.astype(BF16)

        def fetch_o(t, i, wide):
            col, width = span_o(t, i, wide)
            return fetch_d(g_o, r_o, col, width, i) + [
                pltpu.make_async_copy(x.at[:, pl.ds(col, width)], ys.at[i, :, pl.ds(0, width)], xsem.at[i])]

        def put_o(t, i, wide):
            col, width = span_o(t, i, wide)
            return pltpu.make_async_copy(ys.at[i, :, pl.ds(0, width)], y.at[:, pl.ds(col, width)], ysem.at[i])

        def project(t, i):
            in_round(t, lambda wide: wait(fetch_o(t, i, wide)))

            @pl.loop(0, WIDE // NARROW - lax.div(t - first_o, n_wide))
            def _(n):
                c = pl.ds(pl.multiple_of(n * NARROW, NARROW), NARROW)

                @pl.loop(0, T // ROWS)
                def _(m):
                    r = rows_of(m, ROWS)
                    acc = jnp.dot(act[r, :], wbuf[i, :, :, c].reshape(H * VD, NARROW), preferred_element_type=F32)
                    ys[i, r, c] = (ys[i, r, c].astype(F32) + acc).astype(BF16)
            in_round(t, lambda wide: put_o(t, i, wide).start())

        def piece(t, i):
            if not isinstance(t, int):
                if i < 2:
                    project(t, i)
            elif t == 0:
                if i == 0:
                    norm_tokens()
                elif i == 1:
                    kv_down()
                    start(fetch_d(g_dq, r_d, 0, WIDE, 0))
                else:
                    q_down(0)
                    start(fetch_d(g_dq, r_d, 2 * WIDE, WIDE, 0))
            elif t == 1 and i < 2:
                q_down(1 + i)
            elif 2 <= t < first_o and i < 2:
                k0 = (t - 2) * 4 + i * 2
                pl.loop(k0, k0 + 2)(lambda k: heads(k, k < (t - 2) * 4 + 3))

        def prefetch(t):
            if not isinstance(t, int):
                for i in range(2):
                    @pl.when(t > first_o)
                    def _():
                        in_round(t - 1, lambda wide: put_o(t - 1, i, wide).wait())
                    in_round(t, lambda wide: start(fetch_o(t, i, wide)))
            elif t == 1:
                start(fetch_d(g_dq, r_d, WIDE, WIDE, 1))
            elif 2 <= t < first_o:
                start(fetch_u((t - 2) * 4))
            elif t == first_o:
                for i in range(2):
                    start(fetch_o(t, i, True))

        def tick(t):
            comm(t + 1, S1)
            comm(t, S2)
            piece(t - 2, 0)
            comm(t - 1, S4)
            comm(t, S3)
            piece(t - 2, 1)
            comm(t - 1, S5)
            comm(t - 1, S6)
            prefetch(t - 1)
            piece(t - 2, 2)

        comm(0, S1)
        wait(stage_in)
        start(stage_out)
        wait(stage_out)
        for t in range(first_o + 2):
            tick(t)
        pl.loop(first_o + 2, n_rounds + 2)(tick)

        pltpu.make_async_copy(cl, lat, loc.at[1]).wait()
        pltpu.make_async_copy(rr, kpe, loc.at[2]).wait()
        for r in fixed:
            for c in r:
                for j in range(12):
                    copy_of(c, j).wait_send()

        for lo, hi, wide in ((first_o, last_wide, True), (last_wide, n_rounds, False)):
            @pl.loop(lo, hi)
            def _(t):
                for c in chunks(t, wide):
                    for j in range(12):
                        copy_of(c, j).wait_send()

    n_chunks = 5 + 2 * n_groups + 2 * (n_wide + 2)
    gathered = lambda r, c: jax.ShapeDtypeStruct((side, side, CORES, r, c), BF16)
    lanes_gp = math.lcm(r_d, LANES)
    out_shape = [jax.ShapeDtypeStruct((T, D), BF16), jax.ShapeDtypeStruct((T, KVR), BF16),
                 jax.ShapeDtypeStruct((T, LANES), BF16), gathered(16, lanes_gp), gathered(r_d, KVR + LANES),
                 gathered(r_d, QR), gathered(r_q, n_groups * GW), gathered(r_kv, n_groups * KVW), gathered(r_o, D)]
    scratch = [pltpu.VMEM((T, H * VD), BF16), pltpu.VMEM((T, QR), BF16), pltpu.VMEM((T, KVR), BF16),
               pltpu.VMEM((T, LANES), BF16), pltpu.VMEM((T, QR), F32), pltpu.VMEM((2, n_dev, r_o, WIDE), BF16),
               pltpu.VMEM((2, 64, D), BF16),
               pltpu.VMEM((2, side, side, CORES, r_q, HALF * (NOPE + RD)), BF16),
               pltpu.VMEM((2, side, side, CORES, r_kv, HALF * (NOPE + VD)), BF16),
               pltpu.VMEM((HROWS, HALF * NOPE), BF16), pltpu.VMEM((HROWS, HALF * RD), BF16),
               pltpu.VMEM((HROWS, HALF * (NOPE + VD)), BF16), pltpu.VMEM((2, T, WIDE), BF16),
               pltpu.VMEM((side, side, CORES, 16, lanes_gp), BF16),
               pltpu.VMEM((16, lanes_gp), BF16), pltpu.VMEM((r_d, KVR + LANES), BF16), pltpu.VMEM((r_d, QR), BF16),
               pltpu.VMEM((r_q, n_groups * GW), BF16), pltpu.VMEM((r_kv, n_groups * KVW), BF16),
               pltpu.SemaphoreType.DMA((n_chunks, 12)), pltpu.SemaphoreType.DMA((n_chunks, 12)),
               pltpu.SemaphoreType.DMA((3,)), pltpu.SemaphoreType.DMA((2, 5 + D // WIDE)),
               pltpu.SemaphoreType.DMA((2, side * side)), pltpu.SemaphoreType.DMA((2, 2)),
               pltpu.SemaphoreType.DMA((2,)), pltpu.SemaphoreType.DMA((2,))]
    return kernel, out_shape, scratch


def hand_over(y_ref, lat_ref, kpe_ref, y_out, lat_out, kpe_out):
    y_out[...] = y_ref[...]
    lat_out[...] = lat_ref[...]
    kpe_out[...] = kpe_ref[:, :kpe_out.shape[1]]


def solution(mesh):
    batch_spec = P(('dp', 'fsdp'))
    row_spec = P('fsdp')
    mat_spec = P('fsdp', None)
    n_dev = mesh.shape['fsdp']

    def run_block(tokens, gain_in, w_dq, gain_q, w_uq, w_dkv, gain_kv, w_ukv, w_out):
        D, QR = w_dq.shape
        KVR = gain_kv.shape[0]
        RD = w_dkv.shape[1] - KVR
        nope_total = w_ukv.shape[1] - w_out.shape[0]
        H = (w_uq.shape[1] - nope_total) // RD
        NOPE, VD = nope_total // H, w_out.shape[0] // H
        SEQ = tokens.shape[1]

        def local_block(tok, gin, wdq, gq, wuq, wdkv, gkv, wukv, wo):
            n_prompts = tok.shape[0]
            T = n_prompts * SEQ
            kernel, out_shape, scratch = make_kernel(n_dev, (T, D, QR, KVR, H, NOPE, RD, VD, SEQ))
            me = lax.axis_index('fsdp')
            pack = jnp.zeros((16, math.lcm(D // n_dev, LANES)), BF16)
            for row, g in enumerate((gin, gq, gkv)):
                period = math.lcm(g.shape[0], LANES) // g.shape[0]
                pack = lax.dynamic_update_slice(pack, g[None, :], (row, lax.rem(me, period) * g.shape[0]))
            wdkv2 = jnp.concatenate([wdkv] + [wdkv[:, KVR:]] * (LANES // RD - 1), axis=1)
            tables = rope_tables(SEQ, RD)
            cmask = np.tril(np.ones((SEQ, SEQ), np.float32))
            lmask = np.zeros((LANES // RD, 1, LANES), np.float32)
            for j in range(LANES // RD):
                lmask[j, 0, j * RD:(j + 1) * RD] = 1
            hbm = pl.BlockSpec(memory_space=pltpu.HBM)
            vmem = pl.BlockSpec(memory_space=pltpu.VMEM)
            outs = pl.pallas_call(
                kernel,
                name="mla",
                out_shape=out_shape,
                in_specs=[hbm] * 7 + [vmem] * 5,
                out_specs=[hbm] * len(out_shape),
                scratch_shapes=scratch,
                compiler_params=pltpu.CompilerParams(collective_id=0, has_side_effects=True, vmem_limit_bytes=67043328),
            )(tok.reshape(T, D), pack, wdkv2, wdq, wuq, wukv, wo,
              *[jnp.asarray(t) for t in tables], jnp.asarray(cmask), jnp.asarray(lmask, BF16))
            rows = lambda n: pl.BlockSpec((SEQ, n), lambda i: (i, 0))
            y, lat, kpe = pl.pallas_call(
                hand_over,
                name="hand_over",
                grid=(n_prompts,),
                out_shape=[jax.ShapeDtypeStruct((T, n), BF16) for n in (D, KVR, RD)],
                in_specs=[rows(D), rows(KVR), rows(LANES)],
                out_specs=[rows(D), rows(KVR), rows(RD)],
            )(*outs[:3])
            return y.reshape(tok.shape), lat.reshape(n_prompts, SEQ, KVR), kpe.reshape(n_prompts, SEQ, RD)

        mapped = jax.shard_map(
            local_block,
            mesh=mesh,
            in_specs=(batch_spec, row_spec, mat_spec, row_spec, mat_spec, mat_spec, row_spec, mat_spec, mat_spec),
            out_specs=(batch_spec, batch_spec, batch_spec),
            check_vma=False,
        )
        return mapped(tokens, gain_in, w_dq, gain_q, w_uq, w_dkv, gain_kv, w_ukv, w_out)

    return run_block
```
